256 devices in a mesh: wide: 32 (over z, x), mom: 8 (over y, core).
Axes of the slice: x: 4, y: 4, z: 8, core: 2. Of those that a mesh axis runs over, the one named last changes fastest.
Arguments:
- green_blocks: bfloat16 [64, 8, 1024, 256], P('wide', 'mom'), may hold values from -6 to 6
- neighbours: int32 [1024, 4], P(('wide', 'mom')), may hold values from 0 to 1023, as said below
- counts: int32 [1024], P(('wide', 'mom')), may hold values from 1 to 4, as said below
- couplings: float32 [1024, 4, 8, 4], P(('wide', 'mom')), may hold values from 0.01 to 0.1
- grad_h: bfloat16 [1024, 4, 16, 16], P(('wide', 'mom')), may hold values from -1.5 to 1.5
- momentum_table: int32 [8, 8], replicated, may hold values from 0 to 7, each once within a row
Outputs:
- self_energy: bfloat16 [64, 8, 1024, 256], P('wide', 'mom')
The draws below stay inside these ranges and needn't reach their ends.
Inputs may be any that keep to these rules, and one draw needn't show every extreme that they name: `neighbours`: the first counts[a] slots of row a hold distinct atoms other than a, each within 2 positions of a; the remaining slots hold a itself. `counts`: some atom uses all 4 slots. `momentum_table`: each row is a permutation of the momentum points.
All inputs are finite; a program needn't handle non-finite values.
Results may differ from the reference program's by a relative error of at most 0.0064.
Values may be sent and summed in bfloat16 or wider, within the bound.
No kernel may reach another device: no remote copies, remote signals or barrier semaphores. Data moves between devices by JAX's collectives and lax.ppermute only.
A program may use at most 64 MiB of HBM per device.

```python
import math
import jax
import jax.numpy as jnp
from jax import lax

NO = 16
NK = 8
REACH = 2
NW = 2
ESTEP = 3
NB = 4
NE = 64
ATOMS = 1024


def neighbour_tables(key):
    base_key = jax.random.fold_in(key, 7001)
    atom_ids = jnp.arange(ATOMS, dtype=jnp.int32)[:, None]
    offsets = jnp.concatenate([jnp.arange(-REACH, 0, dtype=jnp.int32), jnp.arange(1, REACH + 1, dtype=jnp.int32)])
    candidate = atom_ids + offsets[None, :]
    inside = (candidate >= 0) & (candidate < ATOMS)
    span_size = 2 * REACH
    column_ids = jnp.arange(span_size, dtype=jnp.int32)[None, :]
    scores = jax.random.randint(jax.random.fold_in(base_key, 1), (ATOMS, span_size), 0, 1 << 20) * span_size + column_ids
    scores = jnp.where(inside, scores, (1 << 28) + column_ids)
    ranking = jnp.argsort(scores, axis=1, stable=True)
    chosen = jnp.take_along_axis(candidate, ranking, axis=1)[:, :NB]
    heavy_atom = jax.random.randint(jax.random.fold_in(base_key, 2), (ATOMS,), 0, 4) == 0
    light_count = jax.random.randint(jax.random.fold_in(base_key, 3), (ATOMS,), 1, NB // 2 + 1)
    wanted = jnp.where(heavy_atom, NB, light_count)
    usable = jnp.sum(inside.astype(jnp.int32), axis=1)
    count_values = jnp.minimum(wanted, usable).astype(jnp.int32)
    slot_ids = jnp.arange(NB, dtype=jnp.int32)[None, :]
    neighbour_ids = jnp.where(slot_ids < count_values[:, None], chosen, atom_ids)
    return (neighbour_ids.astype(jnp.int32), count_values)


def draw_neighbours(key, part):
    return neighbour_tables(key)[0]


def draw_counts(key, part):
    return neighbour_tables(key)[1]


def block_levels(key, extent, split, least, top_value):
    loudness, own = 1.0, jax.random.fold_in(key, 6)
    for position, shards_of in split:
        heights = jnp.exp(jax.random.uniform(jax.random.fold_in(own, position), (shards_of,), jnp.float32, least / len(split), top_value / len(split)))
        loudness = loudness * jnp.repeat(heights, extent[position] // shards_of).reshape([-1 if axis == position else 1 for axis in range(len(extent))])
    return loudness


def centred(stream_key, shape, spread, reach, pieces=(), kind=jnp.bfloat16):
    drawn = spread * jax.random.normal(stream_key, shape, jnp.float32)
    if pieces:
        drawn = drawn * block_levels(stream_key, shape, pieces, -0.22, 0.18)
    return jnp.clip(drawn, -reach, reach).astype(kind)


def setup_inputs(seed: int = 0) -> dict:
    streams_of = jax.random.split(jax.random.key(seed), 7)
    green_blocks = centred(streams_of[0], (NE, NK, ATOMS, NO * NO), 1.0, 6.0, ((0, 32), (1, 8)))
    neighbours = draw_neighbours(jax.random.fold_in(streams_of[6], 71), 0)
    counts = draw_counts(jax.random.fold_in(streams_of[6], 71), 0)
    couplings = jnp.clip(jnp.exp(math.log(0.1) - 2.3025851 * jax.random.uniform(streams_of[3], (ATOMS, NB, NK, 2 * NW), jnp.float32) ** block_levels(streams_of[3], (ATOMS, NB, NK, 2 * NW), ((0, 256),), -0.2, 0.2)), 0.01, 0.1)
    grad_h = centred(streams_of[4], (ATOMS, NB, NO, NO), NO ** -0.5, 1.5, ((0, 256),))
    momentum_table = jax.vmap(lambda own: jax.random.permutation(own, NK))(jax.random.split(streams_of[5], NK)).reshape((NK, NK)).astype(jnp.int32)
    return dict(green_blocks=green_blocks, neighbours=neighbours, counts=counts, couplings=couplings, grad_h=grad_h, momentum_table=momentum_table)


def energy_shift(values, amount):
    if amount > 0:
        padding = jnp.zeros((amount,) + values.shape[1:], values.dtype)
        return jnp.concatenate([padding, values[:-amount]], axis=0)
    amount_abs = -amount
    padding = jnp.zeros((amount_abs,) + values.shape[1:], values.dtype)
    return jnp.concatenate([values[amount_abs:], padding], axis=0)


def shift_list(mode_count, spacing):
    upward = [(mode_idx + 1) * spacing for mode_idx in range(mode_count)]
    downward = [-(mode_idx + 1) * spacing for mode_idx in range(mode_count)]
    return upward + downward


def coupling_weights(couplings, counts, momentum_table):
    momenta = momentum_table.shape[0]
    routing = (momentum_table[:, :, None] == jnp.arange(momenta, dtype=jnp.int32)[None, None, :]).astype(jnp.float32)
    slots_used = (jnp.arange(couplings.shape[1], dtype=jnp.int32)[None, :] < counts[:, None]).astype(jnp.float32)
    masked = couplings * slots_used[:, :, None, None]
    combined = jnp.einsum('abqs,kql->abkls', masked, routing, precision=lax.Precision.HIGHEST)
    return combined.astype(jnp.bfloat16)


def kron_blocks(grad_h):
    matrix = grad_h.astype(jnp.float32)
    orbitals = matrix.shape[-1]
    product = matrix[..., :, None, :, None] * matrix[..., None, :, None, :]
    return product.reshape(matrix.shape[:-2] + (orbitals * orbitals, orbitals * orbitals)).astype(jnp.bfloat16)


def reference(green_blocks, neighbours, counts, couplings, grad_h, momentum_table):
    weights = coupling_weights(couplings, counts, momentum_table)
    shifts = shift_list(NW, ESTEP)

    def one_atom(atom_id):
        near_ids = neighbours[atom_id]
        near_blocks = jnp.take(green_blocks, near_ids, axis=2)
        slot_weights = weights[atom_id]
        blended = jnp.zeros(near_blocks.shape, jnp.float32)
        for mode_idx, amount in enumerate(shifts):
            blended = blended + jnp.einsum('bkl,elbx->ekbx', slot_weights[..., mode_idx].astype(jnp.float32), energy_shift(near_blocks, amount).astype(jnp.float32))
        blended = blended.astype(jnp.bfloat16)
        blocks = kron_blocks(grad_h[atom_id])
        summed = jnp.einsum('ekbx,bxy->eky', blended.astype(jnp.float32), blocks.astype(jnp.float32))
        return summed.astype(jnp.bfloat16)

    per_atom = lax.map(one_atom, jnp.arange(ATOMS, dtype=jnp.int32))
    return jnp.transpose(per_atom, (1, 2, 0, 3))
```

```python
import functools

import jax
import jax.numpy as jnp
from jax import lax
from jax.experimental import pallas as pl
from jax.experimental.pallas import tpu as pltpu
from jax.sharding import Mesh, PartitionSpec as P

REACH = 2
NW = 2
ESTEP = 3

NZ, NX, NM = 8, 4, 8
NO = 16
NB = 4
BLOCK = 32
WIDE_BLOCK = BLOCK + 2 * REACH
COLS = 160
UNROLL = 2


def shifts():
    up = [(i + 1) * ESTEP for i in range(NW)]
    return up + [-d for d in up]


def group_exchange(blocks):
    return lax.all_to_all(blocks, ("x", "m"), split_axis=0, concat_axis=0, tiled=True)


def pack_kernel(green_ref, out_ref):
    for m in range(NM):
        for x in range(NX):
            first = (m * NX + x) * BLOCK
            dest = x * NM + m
            halo = []
            for b in range(2):
                out_ref[dest, b * BLOCK : (b + 1) * BLOCK, :] = green_ref[
                    b, first : first + BLOCK, :
                ]
                left = green_ref[b, max(first - 16, 0) : max(first - 16, 0) + 16, :][16 - REACH :]
                after = min(first + BLOCK, 1024 - 16)
                right = green_ref[b, after : after + 16, :][:REACH]
                halo += [left, right]
            out_ref[dest, 2 * BLOCK :, :] = jnp.concatenate(halo, axis=0)


def packed_blocks(green):
    vmem = pl.BlockSpec(memory_space=pltpu.VMEM)
    return pl.pallas_call(
        pack_kernel,
        out_shape=jax.ShapeDtypeStruct((NX * NM, 2 * WIDE_BLOCK, 256), green.dtype),
        in_specs=[vmem],
        out_specs=vmem,
        cost_estimate=pl.CostEstimate(flops=1 << 22, bytes_accessed=2 << 20, transcendentals=0),
    )(green)


def atom_data(neighbours, counts, couplings, grad_h):
    used = jnp.arange(NB, dtype=jnp.int32)[None, :] < counts[:, None]
    kept = jnp.where(used[:, :, None, None], couplings, 0.0).astype(jnp.bfloat16)
    start = 4 * (
        (lax.axis_index("z") * NX + lax.axis_index("x")) * NM + lax.axis_index("m")
    )
    atoms = start + jnp.arange(4, dtype=jnp.int32)
    offset = (neighbours - atoms[:, None]).astype(jnp.bfloat16)
    rows = jnp.concatenate(
        [
            grad_h.reshape(16, 256),
            kept.reshape(16, 32),
            offset.reshape(16, 1),
            jnp.zeros((16, 95), jnp.bfloat16),
        ],
        axis=1,
    )
    spread = jnp.broadcast_to(rows[None], (NM, 16, 384))
    spread = lax.all_to_all(spread, "m", split_axis=0, concat_axis=0, tiled=True)
    swap = [(z * NM + m, m * NM + z) for z in range(NZ) for m in range(NM)]
    return lax.ppermute(spread, ("z", "m"), swap).reshape(BLOCK * NB, 384)


def banded_weights(kept, momentum_table):
    rows = 2 * NM * 32
    tiled = jnp.tile(kept, (1, 2 * NM))
    lane = jnp.arange(rows, dtype=jnp.int32)
    spread = jnp.where(
        (lane // 32)[None, None, :] == jnp.arange(2 * NM, dtype=jnp.int32)[None, :, None],
        tiled[:, None, :],
        jnp.zeros((), kept.dtype),
    ).reshape(BLOCK * NB * 2 * NM, rows)
    k, b, q, s = lane // 64, lane // 32 % 2, lane // 4 % 8, lane % 4
    shift = jnp.where(s < NW, (s + 1) * ESTEP, (NW - 1 - s) * ESTEP)
    one_hot = (
        jnp.arange(NM, dtype=jnp.int32)[None, :] == k[:, None]
    ).astype(jnp.float32)
    by_k = jnp.dot(one_hot, momentum_table.astype(jnp.float32), precision=lax.Precision.HIGHEST)
    reached = jnp.sum(
        jnp.where(jnp.arange(NM, dtype=jnp.int32)[None, :] == q[:, None], by_k, 0.0), axis=1
    ).astype(jnp.int32)
    column = jnp.arange(NX * 256, dtype=jnp.int32)
    x, inner = column // 256, column % 256
    energy = inner % 80 // 8 * 2 + inner // 80 - NW * ESTEP
    momentum = inner % 8
    chosen = (inner < COLS)[None, :] & (energy[None, :] == (2 * x)[None, :] + (b - shift)[:, None]) & (
        momentum[None, :] == reached[:, None]
    )
    return jnp.dot(spread, chosen.astype(jnp.bfloat16), preferred_element_type=jnp.bfloat16)


def kron_factors(grads):
    lane = jnp.arange(512, dtype=jnp.int32)
    taken = jnp.where(lane < 256, lane // 16, lane % 16)
    pick = (jnp.arange(NO, dtype=jnp.int32)[:, None] == taken[None, :]).astype(jnp.bfloat16)
    return jnp.dot(
        grads.reshape(BLOCK * NB * NO, NO), pick, preferred_element_type=jnp.float32
    )


def atoms_kernel(
    place_ref, below_ref, own_ref, above_ref, weights_ref, factors_ref, out_ref, lanes, near, sums
):
    done = 0
    for part in (below_ref, own_ref, above_ref):

        def widen(i, carry, part=part, done=done):
            rows = part[i].astype(jnp.float32)
            at = pl.multiple_of((done + i) * 72, 8)
            for half in range(2):
                lanes[half, pl.ds(at, 72), :] = rows[:, half * 128 : (half + 1) * 128]
            return carry

        lax.fori_loop(0, part.shape[0], widen, 0, unroll=4)
        done += part.shape[0]

    def regroup(atom, start, step):
        for b in range(2):
            for half in range(2):
                rows = lanes[half, pl.ds(start + b * step, 80, stride=72), :]
                near[atom, b * 80 : (b + 1) * 80, half * 128 : (half + 1) * 128] = rows.astype(
                    jnp.bfloat16
                )

    def regroup_atom(atom, carry):
        regroup(atom, atom, BLOCK)
        return carry

    lax.fori_loop(0, BLOCK, regroup_atom, 0, unroll=2)
    for h in range(2 * REACH):
        regroup(BLOCK + h, 2 * BLOCK + h, 2 * REACH)

    def one_atom(atom):
        total = jnp.zeros((64, 256), jnp.float32)
        for slot in range(NB):
            pair = atom * NB + slot
            row = pl.multiple_of(pair * 16, 16)
            band = jnp.concatenate(
                [weights_ref[pl.ds(row, 16), x * 256 : x * 256 + COLS] for x in range(NX)], axis=0
            )
            blended = jnp.dot(
                band, near[place_ref[pair]], preferred_element_type=jnp.float32
            ).astype(jnp.bfloat16)
            factors = factors_ref[pl.ds(row, 16), :]
            each, whole = factors[:, :256], factors[:, 256:]
            kron = jnp.concatenate(
                [(each[i : i + 1, :] * whole).astype(jnp.bfloat16) for i in range(NO)], axis=0
            )
            total = total + jnp.dot(blended, kron, preferred_element_type=jnp.float32)
        for half in range(2):
            sums[half, pl.ds(atom, 64, stride=BLOCK), :] = total[:, half * 128 : (half + 1) * 128]

    def some_atoms(step, carry):
        for i in range(UNROLL):
            one_atom(step * UNROLL + i)
        return carry

    lax.fori_loop(0, BLOCK // UNROLL, some_atoms, 0)

    def narrow(i, carry):
        at = pl.multiple_of(i * 64, 64)
        rows = [sums[half, pl.ds(at, 64), :] for half in range(2)]
        out_ref[i] = jnp.concatenate(rows, axis=1).astype(jnp.bfloat16)
        return carry

    lax.fori_loop(0, NX * NM, narrow, 0, unroll=4)


def self_energy_of(place, below, own, above, weights, factors):
    vmem = pl.BlockSpec(memory_space=pltpu.VMEM)
    flops = 2 * BLOCK * NB * 64 * (COLS + 256) * 256
    return pl.pallas_call(
        atoms_kernel,
        out_shape=jax.ShapeDtypeStruct((NX * NM, 2 * BLOCK, 256), jnp.bfloat16),
        in_specs=[pl.BlockSpec(memory_space=pltpu.SMEM)] + [vmem] * 5,
        out_specs=vmem,
        scratch_shapes=[
            pltpu.VMEM((2, 80 * 72, 128), jnp.float32),
            pltpu.VMEM((WIDE_BLOCK, COLS, 256), jnp.bfloat16),
            pltpu.VMEM((2, 2048, 128), jnp.float32),
        ],
        cost_estimate=pl.CostEstimate(flops=flops, bytes_accessed=16 << 20, transcendentals=0),
        compiler_params=pltpu.CompilerParams(vmem_limit_bytes=48 << 20),
    )(place, below, own, above, weights, factors)


def body(green_blocks, neighbours, counts, couplings, grad_h, momentum_table):
    own = group_exchange(packed_blocks(green_blocks.reshape(2, 1024, 256)))
    up = [(i, i + 1) for i in range(NZ - 1)]
    below = lax.ppermute(own[NM:], "z", up)
    above = lax.ppermute(own[:-NM], "z", [(b, a) for a, b in up])

    data = atom_data(neighbours, counts, couplings, grad_h)
    weights = banded_weights(data[:, 256:288], momentum_table)
    factors = kron_factors(data[:, :256])
    offset = data[:, 288].astype(jnp.float32).astype(jnp.int32)
    spot = jnp.arange(BLOCK * NB, dtype=jnp.int32) // NB + offset
    place = jnp.where(spot < 0, BLOCK + REACH + spot, jnp.where(spot < BLOCK, spot, REACH + spot))
    place = jnp.clip(place, 0, WIDE_BLOCK - 1)

    result = self_energy_of(place, below, own, above, weights, factors)
    back = group_exchange(result)
    back = back.reshape(NX, NM, 2, BLOCK, 256).transpose(2, 1, 0, 3, 4)
    return back.reshape(2, 1, 1024, 256)


def solution(mesh):
    cube = Mesh(mesh.devices.reshape(NZ, NX, NM), ("z", "x", "m"))
    flat = ("z", "x", "m")
    in_specs = (
        P(("z", "x"), "m", None, None),
        P(flat, None),
        P(flat),
        P(flat, None, None, None),
        P(flat, None, None, None),
        P(),
    )
    out_specs = P(("z", "x"), "m", None, None)
    return jax.shard_map(body, mesh=cube, in_specs=in_specs, out_specs=out_specs, check_vma=False)
```

```python
import jax
import jax.numpy as jnp
from jax import lax
from jax.experimental import pallas as pl
from jax.experimental.pallas import tpu as pltpu
from jax.sharding import Mesh, PartitionSpec as P


REACH = 2
NW = 2
ESTEP = 3

NZ, NX, NM = 8, 4, 8
NO = 16
NB = 4
BLOCK = 32
WIDE_BLOCK = BLOCK + 2 * REACH
COLS = 160
UNROLL = 2
IN_STRIDE, OUT_STRIDE = 76, 36


def group_exchange(blocks):
    return lax.all_to_all(blocks, ("x", "m"), split_axis=0, concat_axis=0, tiled=True)


def pack_kernel(green_ref, out_ref):
    for m in range(NM):
        for x in range(NX):
            first = (m * NX + x) * BLOCK
            dest = x * NM + m
            halo = []
            for b in range(2):
                out_ref[dest, b * BLOCK : (b + 1) * BLOCK, :] = green_ref[
                    b, first : first + BLOCK, :
                ]
                left = green_ref[b, max(first - 16, 0) : max(first - 16, 0) + 16, :][16 - REACH :]
                after = min(first + BLOCK, 1024 - 16)
                right = green_ref[b, after : after + 16, :][:REACH]
                halo += [left, right]
            out_ref[dest, 2 * BLOCK :, :] = jnp.concatenate(halo, axis=0)


def packed_blocks(green):
    vmem = pl.BlockSpec(memory_space=pltpu.VMEM)
    return pl.pallas_call(
        pack_kernel,
        out_shape=jax.ShapeDtypeStruct((NX * NM, 2 * WIDE_BLOCK, 256), green.dtype),
        in_specs=[vmem],
        out_specs=vmem,
        cost_estimate=pl.CostEstimate(flops=1 << 22, bytes_accessed=2 << 20, transcendentals=0),
        compiler_params=pltpu.CompilerParams(vmem_limit_bytes=8 << 20),
    )(green)


def atom_data(neighbours, counts, couplings, grad_h):
    used = jnp.arange(NB, dtype=jnp.int32)[None, :] < counts[:, None]
    kept = jnp.where(used[:, :, None, None], couplings, 0.0).astype(jnp.bfloat16)
    start = 4 * (
        (lax.axis_index("z") * NX + lax.axis_index("x")) * NM + lax.axis_index("m")
    )
    atoms = start + jnp.arange(4, dtype=jnp.int32)
    offset = (neighbours - atoms[:, None]).astype(jnp.bfloat16)
    rows = jnp.concatenate(
        [
            grad_h.reshape(16, 256),
            kept.reshape(16, 32),
            offset.reshape(16, 1),
            jnp.zeros((16, 95), jnp.bfloat16),
        ],
        axis=1,
    )
    held = rows[None]
    for step in range(3):
        pairs = [(z, z ^ (1 << step)) for z in range(NZ)]
        held = jnp.concatenate([held, lax.ppermute(held, "z", pairs)], axis=0)
    for step in range(3):
        bit = (lax.axis_index("z") >> step) & 1
        split = held.reshape(NZ >> (step + 1), 2, 1 << step, 16, 384)
        held = jnp.where(bit == 1, jnp.flip(split, axis=1), split).reshape(NZ, 16, 384)
    return held


def group_data(held):
    mine = lax.all_to_all(held, "m", split_axis=0, concat_axis=0, tiled=True)
    return mine.reshape(BLOCK * NB, 384)


def banded_weights(kept, momentum_table):
    rows = 2 * NM * 32
    tiled = jnp.tile(kept, (1, 2 * NM))
    lane = jnp.arange(rows, dtype=jnp.int32)
    spread = jnp.where(
        (lane // 32)[None, None, :] == jnp.arange(2 * NM, dtype=jnp.int32)[None, :, None],
        tiled[:, None, :],
        jnp.zeros((), kept.dtype),
    ).reshape(BLOCK * NB * 2 * NM, rows)
    k, b, q, s = lane // 64, lane // 32 % 2, lane // 4 % 8, lane % 4
    shift = jnp.where(s < NW, (s + 1) * ESTEP, (NW - 1 - s) * ESTEP)
    one_hot = (
        jnp.arange(NM, dtype=jnp.int32)[None, :] == k[:, None]
    ).astype(jnp.float32)
    by_k = jnp.dot(one_hot, momentum_table.astype(jnp.float32), precision=lax.Precision.HIGHEST)
    reached = jnp.sum(
        jnp.where(jnp.arange(NM, dtype=jnp.int32)[None, :] == q[:, None], by_k, 0.0), axis=1
    ).astype(jnp.int32)
    column = jnp.arange(NX * 256, dtype=jnp.int32)
    x, inner = column // 256, column % 256
    energy = inner % 80 // 8 * 2 + inner // 80 - NW * ESTEP
    momentum = inner % 8
    chosen = (inner < COLS)[None, :] & (energy[None, :] == (2 * x)[None, :] + (b - shift)[:, None]) & (
        momentum[None, :] == reached[:, None]
    )
    return jnp.dot(spread, chosen.astype(jnp.bfloat16), preferred_element_type=jnp.bfloat16)


def kron_factors(grads):
    lane = jnp.arange(512, dtype=jnp.int32)
    taken = jnp.where(lane < 256, lane // 16, lane % 16)
    pick = (jnp.arange(NO, dtype=jnp.int32)[:, None] == taken[None, :]).astype(jnp.bfloat16)
    return jnp.dot(
        grads.reshape(BLOCK * NB * NO, NO), pick, preferred_element_type=jnp.float32
    )


def atoms_kernel(
    place_ref, below_ref, own_ref, above_ref, weights_ref, factors_ref, out_ref, lanes, near, sums
):
    done = 0
    for part in (below_ref, own_ref, above_ref):

        def widen(i, carry, part=part, done=done):
            rows = part[i].astype(jnp.float32)
            at = pl.multiple_of((done + i) * IN_STRIDE, 4)
            for half in range(2):
                lanes[half, pl.ds(at, 72), :] = rows[:, half * 128 : (half + 1) * 128]
            return carry

        lax.fori_loop(0, part.shape[0], widen, 0, unroll=4)
        done += part.shape[0]

    def regroup(atom, start, step):
        for b in range(2):
            for half in range(2):
                rows = lanes[half, pl.ds(start + b * step, 80, stride=IN_STRIDE), :]
                near[atom, b * 80 : (b + 1) * 80, half * 128 : (half + 1) * 128] = rows.astype(
                    jnp.bfloat16
                )

    def regroup_atom(atom, carry):
        regroup(atom, atom, BLOCK)
        return carry

    lax.fori_loop(0, BLOCK, regroup_atom, 0, unroll=2)
    for h in range(2 * REACH):
        regroup(BLOCK + h, 2 * BLOCK + h, 2 * REACH)

    def one_atom(atom):
        total = jnp.zeros((64, 256), jnp.float32)
        for slot in range(NB):
            pair = atom * NB + slot
            row = pl.multiple_of(pair * 16, 16)
            band = jnp.concatenate(
                [weights_ref[pl.ds(row, 16), x * 256 : x * 256 + COLS] for x in range(NX)], axis=0
            )
            blended = jnp.dot(
                band, near[place_ref[pair]], preferred_element_type=jnp.float32
            ).astype(jnp.bfloat16)
            factors = factors_ref[pl.ds(row, 16), :]
            each, whole = factors[:, :256], factors[:, 256:]
            kron = jnp.concatenate(
                [(each[i : i + 1, :] * whole).astype(jnp.bfloat16) for i in range(NO)], axis=0
            )
            total = total + jnp.dot(blended, kron, preferred_element_type=jnp.float32)
        for half in range(2):
            sums[half, pl.ds(atom, 64, stride=OUT_STRIDE), :] = total[:, half * 128 : (half + 1) * 128]

    def some_atoms(step, carry):
        for i in range(UNROLL):
            one_atom(step * UNROLL + i)
        return carry

    lax.fori_loop(0, BLOCK // UNROLL, some_atoms, 0)

    def narrow(i, carry):
        for b in range(2):
            at = pl.multiple_of((2 * i + b) * OUT_STRIDE, 4)
            rows = [sums[half, pl.ds(at, BLOCK), :] for half in range(2)]
            out_ref[i, b * BLOCK : (b + 1) * BLOCK, :] = jnp.concatenate(rows, axis=1).astype(
                jnp.bfloat16
            )
        return carry

    lax.fori_loop(0, NX * NM, narrow, 0, unroll=4)


def self_energy_of(place, below, own, above, weights, factors):
    vmem = pl.BlockSpec(memory_space=pltpu.VMEM)
    flops = 2 * BLOCK * NB * 64 * (COLS + 256) * 256
    return pl.pallas_call(
        atoms_kernel,
        out_shape=jax.ShapeDtypeStruct((NX * NM, 2 * BLOCK, 256), jnp.bfloat16),
        in_specs=[pl.BlockSpec(memory_space=pltpu.SMEM)] + [vmem] * 5,
        out_specs=vmem,
        scratch_shapes=[
            pltpu.VMEM((2, 80 * IN_STRIDE, 128), jnp.float32),
            pltpu.VMEM((WIDE_BLOCK, COLS, 256), jnp.bfloat16),
            pltpu.VMEM((2, 64 * OUT_STRIDE, 128), jnp.float32),
        ],
        cost_estimate=pl.CostEstimate(flops=flops, bytes_accessed=16 << 20, transcendentals=0),
        compiler_params=pltpu.CompilerParams(vmem_limit_bytes=24 << 20),
    )(place, below, own, above, weights, factors)


def body(green_blocks, neighbours, counts, couplings, grad_h, momentum_table):
    packed = packed_blocks(green_blocks.reshape(2, 1024, 256))
    packed, neighbours, counts, couplings, grad_h = lax.optimization_barrier(
        (packed, neighbours, counts, couplings, grad_h)
    )
    own = group_exchange(packed)
    up = [(i, i + 1) for i in range(NZ - 1)]
    below = lax.ppermute(own[NM:], "z", up)
    above = lax.ppermute(own[:-NM], "z", [(b, a) for a, b in up])

    held = atom_data(neighbours, counts, couplings, grad_h)
    held, own = lax.optimization_barrier((held, own))
    data = group_data(held)
    weights = banded_weights(data[:, 256:288], momentum_table)
    factors = kron_factors(data[:, :256])
    offset = data[:, 288].astype(jnp.float32).astype(jnp.int32)
    row = jnp.arange(BLOCK * NB, dtype=jnp.int32)
    atom = row // NB
    spot = atom + offset
    place = jnp.where(spot < 0, BLOCK + REACH + spot, jnp.where(spot < BLOCK, spot, REACH + spot))
    place = jnp.clip(place, 0, WIDE_BLOCK - 1)

    result = self_energy_of(place, below, own, above, weights, factors)
    back = group_exchange(result)
    back = back.reshape(NX, NM, 2, BLOCK, 256).transpose(2, 1, 0, 3, 4)
    return back.reshape(2, 1, 1024, 256)


def solution(mesh):
    cube = Mesh(mesh.devices.reshape(NZ, NX, NM), ("z", "x", "m"))
    flat = ("z", "x", "m")
    in_specs = (
        P(("z", "x"), "m", None, None),
        P(flat, None),
        P(flat),
        P(flat, None, None, None),
        P(flat, None, None, None),
        P(),
    )
    out_specs = P(("z", "x"), "m", None, None)
    return jax.shard_map(body, mesh=cube, in_specs=in_specs, out_specs=out_specs, check_vma=False)
```

```python
import jax
import jax.numpy as jnp
from jax import lax
from jax.experimental import pallas as pl
from jax.experimental.pallas import tpu as pltpu
from jax.sharding import Mesh, PartitionSpec as P


REACH = 2
NW = 2
ESTEP = 3

NZ, NX, NM = 8, 4, 8
NO = 16
NB = 4
BLOCK = 32
WIDE_BLOCK = BLOCK + 2 * REACH
COLS = 160
UNROLL = 2
IN_STRIDE, OUT_STRIDE = 76, 34
OFFSETS = (-2, -1, 1, 2)
CHUNK = 32


def group_exchange(blocks):
    return lax.all_to_all(blocks, ("x", "m"), split_axis=0, concat_axis=0, tiled=True)


def pack_kernel(green_ref, out_ref):
    for m in range(NM):
        for x in range(NX):
            first = (m * NX + x) * BLOCK
            dest = x * NM + m
            halo = []
            for b in range(2):
                out_ref[dest, b * BLOCK : (b + 1) * BLOCK, :] = green_ref[
                    b, first : first + BLOCK, :
                ]
                left = green_ref[b, max(first - 16, 0) : max(first - 16, 0) + 16, :][16 - REACH :]
                after = min(first + BLOCK, 1024 - 16)
                right = green_ref[b, after : after + 16, :][:REACH]
                halo += [left, right]
            out_ref[dest, 2 * BLOCK :, :] = jnp.concatenate(halo, axis=0)


def packed_blocks(green):
    vmem = pl.BlockSpec(memory_space=pltpu.VMEM)
    return pl.pallas_call(
        pack_kernel,
        out_shape=jax.ShapeDtypeStruct((NX * NM, 2 * WIDE_BLOCK, 256), green.dtype),
        in_specs=[vmem],
        out_specs=vmem,
        cost_estimate=pl.CostEstimate(flops=1 << 22, bytes_accessed=2 << 20, transcendentals=0),
        compiler_params=pltpu.CompilerParams(vmem_limit_bytes=8 << 20),
    )(green)


def atom_data(neighbours, counts, couplings, grad_h):
    start = 4 * (
        (lax.axis_index("z") * NX + lax.axis_index("x")) * NM + lax.axis_index("m")
    )
    atoms = start + jnp.arange(4, dtype=jnp.int32)
    used = jnp.arange(NB, dtype=jnp.int32)[None, :] < counts[:, None]
    offset = jnp.where(used, neighbours - atoms[:, None], 0)
    wanted = jnp.arange(NB, dtype=jnp.int32) - 2
    wanted = jnp.where(wanted < 0, wanted, wanted + 1)
    here = (offset[:, None, :] == wanted[None, :, None])[..., None, None]
    kept = jnp.sum(jnp.where(here, couplings[:, None], 0.0), axis=2)
    grads = jnp.sum(jnp.where(here, grad_h[:, None].astype(jnp.float32), 0.0), axis=2)
    kept = kept.astype(jnp.bfloat16).reshape(16, 32)
    grads = grads.astype(jnp.bfloat16).reshape(16, 256)
    rows = jnp.concatenate([grads, jnp.tile(kept, (1, NM))], axis=1)
    held = rows[None]
    for step in range(3):
        pairs = [(z, z ^ (1 << step)) for z in range(NZ)]
        held = jnp.concatenate([held, lax.ppermute(held, "z", pairs)], axis=0)
    return held


def sort_kernel(held_ref, out_ref):
    z = lax.axis_index("z")
    for piece in range(NZ):
        out_ref[piece] = held_ref[jnp.bitwise_xor(z, piece)]


def sorted_pieces(held):
    vmem = pl.BlockSpec(memory_space=pltpu.VMEM)
    return pl.pallas_call(
        sort_kernel,
        out_shape=jax.ShapeDtypeStruct(held.shape, held.dtype),
        in_specs=[vmem],
        out_specs=vmem,
        cost_estimate=pl.CostEstimate(flops=1 << 18, bytes_accessed=1 << 18, transcendentals=0),
        compiler_params=pltpu.CompilerParams(vmem_limit_bytes=2 << 20),
    )(held)


def group_data(held):
    mine = lax.all_to_all(sorted_pieces(held), "m", split_axis=0, concat_axis=0, tiled=True)
    return mine.reshape(BLOCK * NB, 512)


def choice_kernel(table_ref, out_ref):
    shape = (32, 512)
    row = lax.broadcasted_iota(jnp.int32, shape, 0)
    column = lax.broadcasted_iota(jnp.int32, shape, 1)
    q, s = row // 4, row % 4
    shift = jnp.where(s < NW, (s + 1) * ESTEP, (NW - 1 - s) * ESTEP)
    inner = column % 256
    energy = inner % 80 // 8 * 2 + inner // 80 - NW * ESTEP
    aim = jnp.where(inner < COLS, energy - column // 256 + shift, -100)
    for k in range(NM):
        reached = jnp.zeros(shape, jnp.int32)
        for place in range(NM):
            reached = jnp.where(q == place, table_ref[k, place], reached)
        same = inner % 8 == reached
        for x in range(NX):
            chosen = jnp.where(same & (aim == 2 * x), 1.0, 0.0)
            out_ref[k * 32 : (k + 1) * 32, x * 512 : (x + 1) * 512] = chosen.astype(jnp.bfloat16)


def column_choice(momentum_table):
    return pl.pallas_call(
        choice_kernel,
        out_shape=jax.ShapeDtypeStruct((NM * 32, NX * 512), jnp.bfloat16),
        in_specs=[pl.BlockSpec(memory_space=pltpu.SMEM)],
        out_specs=pl.BlockSpec(memory_space=pltpu.VMEM),
        cost_estimate=pl.CostEstimate(flops=1 << 24, bytes_accessed=1 << 20, transcendentals=0),
        compiler_params=pltpu.CompilerParams(vmem_limit_bytes=4 << 20),
    )(momentum_table)


def weights_kernel(data_ref, choice_ref, out_ref, factors_ref):
    lane = lax.broadcasted_iota(jnp.int32, (NM, 256), 1)
    mine = lane // 32 == lax.broadcasted_iota(jnp.int32, (NM, 256), 0)
    lane = lax.broadcasted_iota(jnp.int32, (NO, 256), 1)
    in_row = lane // NO == lax.broadcasted_iota(jnp.int32, (NO, 256), 0)
    entry = lax.broadcasted_iota(jnp.int32, (256, 512), 0) % NO
    lane = lax.broadcasted_iota(jnp.int32, (256, 512), 1)
    taken = jnp.where(lane < 256, lane // NO, lane % NO)
    pick = jnp.where(entry == taken, 1.0, 0.0).astype(jnp.bfloat16)

    def some_pairs(step, carry):
        at = pl.multiple_of(step * CHUNK, CHUNK)
        kept = data_ref[pl.ds(at, CHUNK), 256:512].astype(jnp.float32)
        rows = [jnp.where(mine, kept[i : i + 1, :], 0.0) for i in range(CHUNK)]
        spread = jnp.concatenate(rows, axis=0).astype(jnp.bfloat16)
        for x in range(NX):
            both = [
                jnp.dot(
                    spread,
                    choice_ref[:, (2 * x + b) * 256 : (2 * x + b + 1) * 256],
                    preferred_element_type=jnp.float32,
                ).reshape(CHUNK, NM, 256)
                for b in range(2)
            ]
            out_ref[pl.ds(at, CHUNK), x * 16 : (x + 1) * 16, :] = jnp.concatenate(
                both, axis=1
            ).astype(jnp.bfloat16)
        grads = data_ref[pl.ds(at, CHUNK), :256].astype(jnp.float32)
        rows = [jnp.where(in_row, grads[i : i + 1, :], 0.0) for i in range(CHUNK)]
        factors_ref[pl.ds(pl.multiple_of(at * NO, CHUNK * NO), CHUNK * NO), :] = jnp.dot(
            jnp.concatenate(rows, axis=0).astype(jnp.bfloat16),
            pick,
            preferred_element_type=jnp.float32,
        )
        return carry

    lax.fori_loop(0, BLOCK * NB // CHUNK, some_pairs, 0)


def weights_and_factors(data, choice):
    vmem = pl.BlockSpec(memory_space=pltpu.VMEM)
    return pl.pallas_call(
        weights_kernel,
        out_shape=[
            jax.ShapeDtypeStruct((BLOCK * NB, 64, 256), jnp.bfloat16),
            jax.ShapeDtypeStruct((BLOCK * NB * NO, 512), jnp.float32),
        ],
        in_specs=[vmem, vmem],
        out_specs=[vmem, vmem],
        cost_estimate=pl.CostEstimate(flops=1 << 30, bytes_accessed=6 << 20, transcendentals=0),
        compiler_params=pltpu.CompilerParams(vmem_limit_bytes=16 << 20),
    )(data, choice)


def atoms_kernel(
    below_ref, own_ref, above_ref, weights_ref, factors_ref, out_ref, lanes, near, blend, sums
):
    done = 0
    for part in (below_ref, own_ref, above_ref):

        def widen(i, carry, part=part, done=done):
            rows = part[i].astype(jnp.float32)
            at = pl.multiple_of((done + i) * IN_STRIDE, 4)
            for half in range(2):
                lanes[half, pl.ds(at, 72), :] = rows[:, half * 128 : (half + 1) * 128]
            return carry

        lax.fori_loop(0, part.shape[0], widen, 0, unroll=4)
        done += part.shape[0]

    def regroup(place, start, step):
        for b in range(2):
            for half in range(2):
                rows = lanes[half, pl.ds(start + b * step, 80, stride=IN_STRIDE), :]
                near[place, b * 80 : (b + 1) * 80, half * 128 : (half + 1) * 128] = rows.astype(
                    jnp.bfloat16
                )

    def regroup_atom(atom, carry):
        regroup(REACH + atom, atom, BLOCK)
        return carry

    lax.fori_loop(0, BLOCK, regroup_atom, 0, unroll=2)
    for h in range(2 * REACH):
        regroup(h if h < REACH else BLOCK + h, 2 * BLOCK + h, 2 * REACH)

    def blend_from(place, carry):
        bands = []
        for d, offset in enumerate(OFFSETS):
            atom = jnp.clip(place - REACH - offset, 0, BLOCK - 1)
            bands.append(weights_ref[atom * NB + d][:, :COLS])
        mixed = jnp.dot(
            jnp.concatenate(bands, axis=0), near[place], preferred_element_type=jnp.float32
        ).astype(jnp.bfloat16)
        for d, offset in enumerate(OFFSETS):
            blend[(place - offset + REACH) * NB + d] = mixed[64 * d : 64 * (d + 1)]
        return carry

    lax.fori_loop(0, WIDE_BLOCK, blend_from, 0, unroll=2)

    def one_atom(atom):
        total = jnp.zeros((64, 256), jnp.float32)
        for d in range(NB):
            pair = atom * NB + d
            factors = factors_ref[pl.ds(pl.multiple_of(pair * 16, 16), 16), :]
            each, whole = factors[:, :256], factors[:, 256:]
            kron = jnp.concatenate(
                [(each[i : i + 1, :] * whole).astype(jnp.bfloat16) for i in range(NO)], axis=0
            )
            total = total + jnp.dot(
                blend[pair + 2 * REACH * NB], kron, preferred_element_type=jnp.float32
            )
        for x in range(NX):
            for b in range(2):
                row = x * 16 + b * 8
                at = (x * 16 + b) * OUT_STRIDE + atom
                for half in range(2):
                    sums[half, pl.ds(at, NM, stride=2 * OUT_STRIDE), :] = total[
                        row : row + NM, half * 128 : (half + 1) * 128
                    ]

    def some_atoms(step, carry):
        for i in range(UNROLL):
            one_atom(step * UNROLL + i)
        return carry

    lax.fori_loop(0, BLOCK // UNROLL, some_atoms, 0)

    def narrow(i, carry):
        for b in range(2):
            at = pl.multiple_of((2 * i + b) * OUT_STRIDE, 2)
            rows = [sums[half, pl.ds(at, BLOCK), :] for half in range(2)]
            out_ref[i, b * BLOCK : (b + 1) * BLOCK, :] = jnp.concatenate(rows, axis=1).astype(
                jnp.bfloat16
            )
        return carry

    lax.fori_loop(0, NX * NM, narrow, 0, unroll=4)


def self_energy_of(below, own, above, weights, factors):
    vmem = pl.BlockSpec(memory_space=pltpu.VMEM)
    flops = 2 * BLOCK * NB * 64 * (COLS + 256) * 256
    return pl.pallas_call(
        atoms_kernel,
        out_shape=jax.ShapeDtypeStruct((NX * NM, 2 * BLOCK, 256), jnp.bfloat16),
        in_specs=[vmem] * 5,
        out_specs=vmem,
        scratch_shapes=[
            pltpu.VMEM((2, 80 * IN_STRIDE, 128), jnp.float32),
            pltpu.VMEM((WIDE_BLOCK, COLS, 256), jnp.bfloat16),
            pltpu.VMEM(((BLOCK + 4 * REACH) * NB, 64, 256), jnp.bfloat16),
            pltpu.VMEM((2, 64 * OUT_STRIDE, 128), jnp.float32),
        ],
        cost_estimate=pl.CostEstimate(flops=flops, bytes_accessed=16 << 20, transcendentals=0),
        compiler_params=pltpu.CompilerParams(vmem_limit_bytes=20 << 20),
    )(below, own, above, weights, factors)


def body(green_blocks, neighbours, counts, couplings, grad_h, momentum_table):
    packed = packed_blocks(green_blocks.reshape(2, 1024, 256))
    packed, neighbours, counts, couplings, grad_h = lax.optimization_barrier(
        (packed, neighbours, counts, couplings, grad_h)
    )
    own = group_exchange(packed)
    up = [(i, i + 1) for i in range(NZ - 1)]
    below = lax.ppermute(own[NM:], "z", up)
    above = lax.ppermute(own[:-NM], "z", [(b, a) for a, b in up])

    held = atom_data(neighbours, counts, couplings, grad_h)
    choice = column_choice(momentum_table)
    held, own, choice = lax.optimization_barrier((held, own, choice))
    data = group_data(held)
    weights, factors = weights_and_factors(data, choice)
    result = self_energy_of(below, own, above, weights, factors)
    back = group_exchange(result)
    back = back.reshape(NX, NM, 2, BLOCK, 256).transpose(2, 1, 0, 3, 4)
    return back.reshape(2, 1, 1024, 256)


def solution(mesh):
    cube = Mesh(mesh.devices.reshape(NZ, NX, NM), ("z", "x", "m"))
    flat = ("z", "x", "m")
    in_specs = (
        P(("z", "x"), "m", None, None),
        P(flat, None),
        P(flat),
        P(flat, None, None, None),
        P(flat, None, None, None),
        P(),
    )
    out_specs = P(("z", "x"), "m", None, None)
    return jax.shard_map(body, mesh=cube, in_specs=in_specs, out_specs=out_specs, check_vma=False)
```

```python
import functools

import jax
import jax.numpy as jnp
from jax import lax
from jax.experimental import pallas as pl
from jax.experimental.pallas import tpu as pltpu
from jax.sharding import Mesh, PartitionSpec as P


REACH = 2
NW = 2
ESTEP = 3

NZ, NX, NM = 8, 4, 8
NO = 16
NB = 4
BLOCK = 32
WIDE_BLOCK = BLOCK + 2 * REACH
COLS = 160
UNROLL = 2
FIRST = 24
EARLY = FIRST + 2 * REACH
LATE = WIDE_BLOCK - EARLY
OFFSETS = (-2, -1, 1, 2)
CHUNK = 32


def group_exchange(blocks):
    return lax.all_to_all(blocks, ("x", "m"), split_axis=0, concat_axis=0, tiled=True)


def pack_kernel(green_ref, out_ref, taken, made, in_sems, out_sems):
    loads = []
    for m in range(NM):
        rows = pl.ds(m * NX * BLOCK, NX * BLOCK)
        copy = pltpu.make_async_copy(green_ref.at[:, rows], taken.at[:, rows], in_sems.at[m])
        copy.start()
        loads.append(copy)
    loads[0].wait()
    stores = []
    for m in range(NM):
        if m + 1 < NM:
            loads[m + 1].wait()
        for x in range(NX):
            first = (m * NX + x) * BLOCK
            before, after = max(first - 16, 0), min(first + BLOCK, 1024 - 16)
            early, late = [], []
            for b in range(2):
                left = taken[b, before : before + 16, :][16 - REACH :]
                right = taken[b, after : after + 16, :][:REACH]
                whole = jnp.concatenate([left, taken[b, first : first + BLOCK, :], right], axis=0)
                early.append(whole[:EARLY])
                late.append(whole[EARLY:])
            dest = x * NM + m
            made[dest] = jnp.concatenate(early + late, axis=0)
            copy = pltpu.make_async_copy(made.at[dest], out_ref.at[dest], out_sems.at[dest])
            copy.start()
            stores.append(copy)
    for copy in stores:
        copy.wait()


def packed_blocks(green):
    shape = (NX * NM, 2 * WIDE_BLOCK, 256)
    return pl.pallas_call(
        pack_kernel,
        out_shape=jax.ShapeDtypeStruct(shape, green.dtype),
        in_specs=[pl.BlockSpec(memory_space=pltpu.HBM)],
        out_specs=pl.BlockSpec(memory_space=pltpu.HBM),
        scratch_shapes=[
            pltpu.VMEM(green.shape, green.dtype),
            pltpu.VMEM(shape, green.dtype),
            pltpu.SemaphoreType.DMA((NM,)),
            pltpu.SemaphoreType.DMA((NX * NM,)),
        ],
        cost_estimate=pl.CostEstimate(flops=1 << 22, bytes_accessed=2 << 20, transcendentals=0),
        compiler_params=pltpu.CompilerParams(vmem_limit_bytes=62 << 20),
    )(green)


def atom_data(neighbours, counts, couplings, grad_h):
    start = 4 * (
        (lax.axis_index("z") * NX + lax.axis_index("x")) * NM + lax.axis_index("m")
    )
    atoms = start + jnp.arange(4, dtype=jnp.int32)
    used = jnp.arange(NB, dtype=jnp.int32)[None, :] < counts[:, None]
    offset = jnp.where(used, neighbours - atoms[:, None], 0)
    wanted = jnp.arange(NB, dtype=jnp.int32) - 2
    wanted = jnp.where(wanted < 0, wanted, wanted + 1)
    here = (offset[:, None, :] == wanted[None, :, None])[..., None, None]
    kept = jnp.sum(jnp.where(here, couplings[:, None], 0.0), axis=2)
    grads = jnp.sum(jnp.where(here, grad_h[:, None].astype(jnp.float32), 0.0), axis=2)
    kept = kept.astype(jnp.bfloat16).reshape(16, 32)
    grads = grads.astype(jnp.bfloat16).reshape(16, 256)
    rows = jnp.concatenate([grads, jnp.tile(kept, (1, NM))], axis=1)
    held = rows[None]
    for step in range(3):
        pairs = [(z, z ^ (1 << step)) for z in range(NZ)]
        held = jnp.concatenate([held, lax.ppermute(held, "z", pairs)], axis=0)
    return held


def sort_kernel(held_ref, out_ref):
    z = lax.axis_index("z")
    for piece in range(NZ):
        out_ref[piece] = held_ref[jnp.bitwise_xor(z, piece)]


def sorted_pieces(held):
    vmem = pl.BlockSpec(memory_space=pltpu.VMEM)
    return pl.pallas_call(
        sort_kernel,
        out_shape=jax.ShapeDtypeStruct(held.shape, held.dtype),
        in_specs=[vmem],
        out_specs=vmem,
        cost_estimate=pl.CostEstimate(flops=1 << 18, bytes_accessed=1 << 18, transcendentals=0),
        compiler_params=pltpu.CompilerParams(vmem_limit_bytes=2 << 20),
    )(held)


def group_data(held):
    mine = lax.all_to_all(sorted_pieces(held), "m", split_axis=0, concat_axis=0, tiled=True)
    return mine.reshape(BLOCK * NB, 512)


def choice_kernel(table_ref, out_ref):
    shape = (32, 512)
    row = lax.broadcasted_iota(jnp.int32, shape, 0)
    column = lax.broadcasted_iota(jnp.int32, shape, 1)
    q, s = row // 4, row % 4
    shift = jnp.where(s < NW, (s + 1) * ESTEP, (NW - 1 - s) * ESTEP)
    inner = column % 256
    energy = inner % 80 // 8 * 2 + inner // 80 - NW * ESTEP
    aim = jnp.where(inner < COLS, energy - column // 256 + shift, -100)
    for k in range(NM):
        reached = jnp.zeros(shape, jnp.int32)
        for place in range(NM):
            reached = jnp.where(q == place, table_ref[k, place], reached)
        same = inner % 8 == reached
        for x in range(NX):
            chosen = jnp.where(same & (aim == 2 * x), 1.0, 0.0)
            out_ref[k * 32 : (k + 1) * 32, x * 512 : (x + 1) * 512] = chosen.astype(jnp.bfloat16)


def column_choice(momentum_table):
    return pl.pallas_call(
        choice_kernel,
        out_shape=jax.ShapeDtypeStruct((NM * 32, NX * 512), jnp.bfloat16),
        in_specs=[pl.BlockSpec(memory_space=pltpu.SMEM)],
        out_specs=pl.BlockSpec(memory_space=pltpu.VMEM),
        cost_estimate=pl.CostEstimate(flops=1 << 24, bytes_accessed=1 << 20, transcendentals=0),
        compiler_params=pltpu.CompilerParams(vmem_limit_bytes=4 << 20),
    )(momentum_table)


def weights_kernel(data_ref, choice_ref, out_ref, factors_ref):
    lane = lax.broadcasted_iota(jnp.int32, (NM, 256), 1)
    mine = lane // 32 == lax.broadcasted_iota(jnp.int32, (NM, 256), 0)
    lane = lax.broadcasted_iota(jnp.int32, (NO, 256), 1)
    in_row = lane // NO == lax.broadcasted_iota(jnp.int32, (NO, 256), 0)
    entry = lax.broadcasted_iota(jnp.int32, (256, 512), 0) % NO
    lane = lax.broadcasted_iota(jnp.int32, (256, 512), 1)
    taken = jnp.where(lane < 256, lane // NO, lane % NO)
    pick = jnp.where(entry == taken, 1.0, 0.0).astype(jnp.bfloat16)

    def some_pairs(step, carry):
        at = pl.multiple_of(step * CHUNK, CHUNK)
        kept = data_ref[pl.ds(at, CHUNK), 256:512].astype(jnp.float32)
        rows = [jnp.where(mine, kept[i : i + 1, :], 0.0) for i in range(CHUNK)]
        spread = jnp.concatenate(rows, axis=0).astype(jnp.bfloat16)
        for x in range(NX):
            both = [
                jnp.dot(
                    spread,
                    choice_ref[:, (2 * x + b) * 256 : (2 * x + b + 1) * 256],
                    preferred_element_type=jnp.float32,
                ).reshape(CHUNK, NM, 256)
                for b in range(2)
            ]
            out_ref[pl.ds(at, CHUNK), x * 16 : (x + 1) * 16, :] = jnp.concatenate(
                both, axis=1
            ).astype(jnp.bfloat16)
        grads = data_ref[pl.ds(at, CHUNK), :256].astype(jnp.float32)
        rows = [jnp.where(in_row, grads[i : i + 1, :], 0.0) for i in range(CHUNK)]
        factors_ref[pl.ds(pl.multiple_of(at * NO, CHUNK * NO), CHUNK * NO), :] = jnp.dot(
            jnp.concatenate(rows, axis=0).astype(jnp.bfloat16),
            pick,
            preferred_element_type=jnp.float32,
        )
        return carry

    lax.fori_loop(0, BLOCK * NB // CHUNK, some_pairs, 0)


def weights_and_factors(data, choice):
    vmem = pl.BlockSpec(memory_space=pltpu.VMEM)
    return pl.pallas_call(
        weights_kernel,
        out_shape=[
            jax.ShapeDtypeStruct((BLOCK * NB, 64, 256), jnp.bfloat16),
            jax.ShapeDtypeStruct((BLOCK * NB * NO, 512), jnp.float32),
        ],
        in_specs=[vmem, vmem],
        out_specs=[vmem, vmem],
        cost_estimate=pl.CostEstimate(flops=1 << 30, bytes_accessed=6 << 20, transcendentals=0),
        compiler_params=pltpu.CompilerParams(vmem_limit_bytes=16 << 20),
    )(data, choice)


def atoms_kernel(begin, end, *refs):
    count = end - begin
    early = begin == 0
    if early:
        below_ref, own_ref, above_ref, weights_ref, factors_ref, out_ref, edge_ref = refs[:7]
        width, skip, known = EARLY, 0, 0
    else:
        below_ref, own_ref, above_ref, weights_ref, factors_ref, edge_ref, ready_ref, out_ref = refs[:8]
        width, skip, known = LATE, 2 * EARLY, 2 * REACH
    lanes, near, blend, sums = refs[-4:]
    stride, out_stride = 2 * width + 4, count + 2

    done = 0
    for part in (below_ref, own_ref, above_ref):
        at_row = skip if part is own_ref else 0

        def widen(i, carry, part=part, done=done, at_row=at_row):
            rows = part[i, at_row : at_row + 2 * width].astype(jnp.float32)
            at = pl.multiple_of((done + i) * stride, 4)
            for half in range(2):
                lanes[half, pl.ds(at, 2 * width), :] = rows[:, half * 128 : (half + 1) * 128]
            return carry

        lax.fori_loop(0, part.shape[0], widen, 0, unroll=4)
        done += part.shape[0]

    def regroup(place, carry):
        for b in range(2):
            for half in range(2):
                rows = lanes[half, pl.ds(place + b * width, 80, stride=stride), :]
                near[known + place, b * 80 : (b + 1) * 80, half * 128 : (half + 1) * 128] = (
                    rows.astype(jnp.bfloat16)
                )
        return carry

    lax.fori_loop(0, width, regroup, 0, unroll=2)
    if early:
        edge_ref[...] = near[count:]
    else:
        near[:known] = edge_ref[...]

    def blend_from(place, carry):
        bands = []
        for d, offset in enumerate(OFFSETS):
            atom = jnp.clip(begin + place - REACH - offset, 0, BLOCK - 1)
            bands.append(weights_ref[atom * NB + d][:, :COLS])
        mixed = jnp.dot(
            jnp.concatenate(bands, axis=0), near[place], preferred_element_type=jnp.float32
        ).astype(jnp.bfloat16)
        for d, offset in enumerate(OFFSETS):
            blend[(place - offset + REACH) * NB + d] = mixed[64 * d : 64 * (d + 1)]
        return carry

    lax.fori_loop(0, count + 2 * REACH, blend_from, 0, unroll=2)

    def one_atom(atom):
        total = jnp.zeros((64, 256), jnp.float32)
        for d in range(NB):
            row = pl.multiple_of(((begin + atom) * NB + d) * NO, NO)
            factors = factors_ref[pl.ds(row, NO), :]
            each, whole = factors[:, :256], factors[:, 256:]
            kron = jnp.concatenate(
                [(each[i : i + 1, :] * whole).astype(jnp.bfloat16) for i in range(NO)], axis=0
            )
            total = total + jnp.dot(
                blend[(atom + 2 * REACH) * NB + d], kron, preferred_element_type=jnp.float32
            )
        for x in range(NX):
            for b in range(2):
                row = x * 16 + b * 8
                at = (x * 16 + b) * out_stride + atom
                for half in range(2):
                    sums[half, pl.ds(at, NM, stride=2 * out_stride), :] = total[
                        row : row + NM, half * 128 : (half + 1) * 128
                    ]

    def some_atoms(step, carry):
        for i in range(UNROLL):
            one_atom(step * UNROLL + i)
        return carry

    lax.fori_loop(0, count // UNROLL, some_atoms, 0)

    def narrow(i, carry):
        for b in range(2):
            at = pl.multiple_of((2 * i + b) * out_stride, 2)
            rows = [sums[half, pl.ds(at, count), :] for half in range(2)]
            rows = jnp.concatenate(rows, axis=1)
            if not early:
                before = ready_ref[i, b * BLOCK : (b + 1) * BLOCK, :].astype(jnp.float32)
                rows = jnp.concatenate([before[:begin], rows], axis=0)
            out_ref[i, b * BLOCK : b * BLOCK + end, :] = rows.astype(jnp.bfloat16)
        return carry

    lax.fori_loop(0, NX * NM, narrow, 0, unroll=4)


def self_energy_of(begin, end, *operands):
    vmem = pl.BlockSpec(memory_space=pltpu.VMEM)
    count = end - begin
    width = EARLY if begin == 0 else LATE
    flops = 2 * count * NB * 64 * (COLS + 256) * 256
    out = jax.ShapeDtypeStruct((NX * NM, 2 * BLOCK, 256), jnp.bfloat16)
    edge = jax.ShapeDtypeStruct((2 * REACH, COLS, 256), jnp.bfloat16)
    return pl.pallas_call(
        functools.partial(atoms_kernel, begin, end),
        out_shape=[out, edge] if begin == 0 else out,
        in_specs=[vmem] * len(operands),
        out_specs=[vmem, vmem] if begin == 0 else vmem,
        scratch_shapes=[
            pltpu.VMEM((2, 80 * (2 * width + 4), 128), jnp.float32),
            pltpu.VMEM((count + 2 * REACH, COLS, 256), jnp.bfloat16),
            pltpu.VMEM(((count + 4 * REACH) * NB, 64, 256), jnp.bfloat16),
            pltpu.VMEM((2, 64 * (count + 2), 128), jnp.float32),
        ],
        cost_estimate=pl.CostEstimate(flops=flops, bytes_accessed=8 << 20, transcendentals=0),
        compiler_params=pltpu.CompilerParams(vmem_limit_bytes=20 << 20),
    )(*operands)


def body(green_blocks, neighbours, counts, couplings, grad_h, momentum_table):
    packed = packed_blocks(green_blocks.reshape(2, 1024, 256))
    packed, neighbours, counts, couplings, grad_h = lax.optimization_barrier(
        (packed, neighbours, counts, couplings, grad_h)
    )
    own = group_exchange(packed)
    up = [(i, i + 1) for i in range(NZ - 1)]
    down = [(b, a) for a, b in up]

    def exchanged(rows):
        below = lax.ppermute(own[NM:, rows], "z", up)
        above = lax.ppermute(own[:-NM, rows], "z", down)
        return below, above

    below, above = exchanged(slice(0, 2 * EARLY))
    held = atom_data(neighbours, counts, couplings, grad_h)
    choice = column_choice(momentum_table)
    held, own, choice = lax.optimization_barrier((held, own, choice))
    data = group_data(held)
    data, own = lax.optimization_barrier((data, own))
    late_below, late_above = exchanged(slice(2 * EARLY, 2 * WIDE_BLOCK))
    weights, factors = weights_and_factors(data, choice)
    result, edge = self_energy_of(
        0, FIRST, below, own, above, weights, factors
    )
    result = self_energy_of(
        FIRST, BLOCK, late_below, own, late_above, weights, factors, edge, result
    )
    back = group_exchange(result)
    back = back.reshape(NX, NM, 2, BLOCK, 256).transpose(2, 1, 0, 3, 4)
    return back.reshape(2, 1, 1024, 256)


def solution(mesh):
    cube = Mesh(mesh.devices.reshape(NZ, NX, NM), ("z", "x", "m"))
    flat = ("z", "x", "m")
    in_specs = (
        P(("z", "x"), "m", None, None),
        P(flat, None),
        P(flat),
        P(flat, None, None, None),
        P(flat, None, None, None),
        P(),
    )
    out_specs = P(("z", "x"), "m", None, None)
    return jax.shard_map(body, mesh=cube, in_specs=in_specs, out_specs=out_specs, check_vma=False)
```

```python
import functools

import jax
import jax.numpy as jnp
from jax import lax
from jax.experimental import pallas as pl
from jax.experimental.pallas import tpu as pltpu
from jax.sharding import Mesh, PartitionSpec as P


REACH = 2
NW = 2
ESTEP = 3

NZ, NX, NM = 8, 4, 8
NO = 16
NB = 4
BLOCK = 32
WIDE_BLOCK = BLOCK + 2 * REACH
COLS = 160
UNROLL = 8
FIRST = 24
EARLY = FIRST + 2 * REACH
LATE = WIDE_BLOCK - EARLY
OFFSETS = (-2, -1, 1, 2)
CHUNK = 32


def group_exchange(blocks):
    return lax.all_to_all(blocks, ("x", "m"), split_axis=0, concat_axis=0, tiled=True)


def pack_kernel(green_ref, out_ref, taken, made, in_sems, out_sems):
    loads = []
    for m in range(NM):
        rows = pl.ds(m * NX * BLOCK, NX * BLOCK)
        copy = pltpu.make_async_copy(green_ref.at[:, rows], taken.at[:, rows], in_sems.at[m])
        copy.start()
        loads.append(copy)
    loads[0].wait()
    stores = []
    for m in range(NM):
        if m + 1 < NM:
            loads[m + 1].wait()
        for x in range(NX):
            first = (m * NX + x) * BLOCK
            before, after = max(first - 16, 0), min(first + BLOCK, 1024 - 16)
            early, late = [], []
            for b in range(2):
                left = taken[b, before : before + 16, :][16 - REACH :]
                right = taken[b, after : after + 16, :][:REACH]
                whole = jnp.concatenate([left, taken[b, first : first + BLOCK, :], right], axis=0)
                early.append(whole[:EARLY])
                late.append(whole[EARLY:])
            dest = x * NM + m
            made[dest] = jnp.concatenate(early + late, axis=0)
            copy = pltpu.make_async_copy(made.at[dest], out_ref.at[dest], out_sems.at[dest])
            copy.start()
            stores.append(copy)
    for copy in stores:
        copy.wait()


def packed_blocks(green):
    shape = (NX * NM, 2 * WIDE_BLOCK, 256)
    return pl.pallas_call(
        pack_kernel,
        out_shape=jax.ShapeDtypeStruct(shape, green.dtype),
        in_specs=[pl.BlockSpec(memory_space=pltpu.HBM)],
        out_specs=pl.BlockSpec(memory_space=pltpu.HBM),
        scratch_shapes=[
            pltpu.VMEM(green.shape, green.dtype),
            pltpu.VMEM(shape, green.dtype),
            pltpu.SemaphoreType.DMA((NM,)),
            pltpu.SemaphoreType.DMA((NX * NM,)),
        ],
        cost_estimate=pl.CostEstimate(flops=1 << 22, bytes_accessed=2 << 20, transcendentals=0),
        compiler_params=pltpu.CompilerParams(vmem_limit_bytes=62 << 20),
    )(green)


def atom_data(neighbours, counts, couplings, grad_h):
    start = 4 * (
        (lax.axis_index("z") * NX + lax.axis_index("x")) * NM + lax.axis_index("m")
    )
    atoms = start + jnp.arange(4, dtype=jnp.int32)
    used = jnp.arange(NB, dtype=jnp.int32)[None, :] < counts[:, None]
    offset = jnp.where(used, neighbours - atoms[:, None], 0)
    wanted = jnp.arange(NB, dtype=jnp.int32) - 2
    wanted = jnp.where(wanted < 0, wanted, wanted + 1)
    here = (offset[:, None, :] == wanted[None, :, None])[..., None, None]
    kept = jnp.sum(jnp.where(here, couplings[:, None], 0.0), axis=2)
    grads = jnp.sum(jnp.where(here, grad_h[:, None].astype(jnp.float32), 0.0), axis=2)
    kept = kept.astype(jnp.bfloat16).reshape(16, 32)
    grads = grads.astype(jnp.bfloat16).reshape(16, 256)
    rows = jnp.concatenate([grads, jnp.tile(kept, (1, NM))], axis=1)
    held = rows[None]
    for step in range(3):
        pairs = [(z, z ^ (1 << step)) for z in range(NZ)]
        held = jnp.concatenate([held, lax.ppermute(held, "z", pairs)], axis=0)
    return held


def sort_kernel(held_ref, out_ref):
    z = lax.axis_index("z")
    for piece in range(NZ):
        out_ref[piece] = held_ref[jnp.bitwise_xor(z, piece)]


def sorted_pieces(held):
    vmem = pl.BlockSpec(memory_space=pltpu.VMEM)
    return pl.pallas_call(
        sort_kernel,
        out_shape=jax.ShapeDtypeStruct(held.shape, held.dtype),
        in_specs=[vmem],
        out_specs=vmem,
        cost_estimate=pl.CostEstimate(flops=1 << 18, bytes_accessed=1 << 18, transcendentals=0),
        compiler_params=pltpu.CompilerParams(vmem_limit_bytes=2 << 20),
    )(held)


def group_data(held):
    mine = lax.all_to_all(sorted_pieces(held), "m", split_axis=0, concat_axis=0, tiled=True)
    return mine.reshape(BLOCK * NB, 512)


def choice_kernel(table_ref, out_ref):
    shape = (32, 512)
    row = lax.broadcasted_iota(jnp.int32, shape, 0)
    column = lax.broadcasted_iota(jnp.int32, shape, 1)
    q, s = row // 4, row % 4
    shift = jnp.where(s < NW, (s + 1) * ESTEP, (NW - 1 - s) * ESTEP)
    inner = column % 256
    energy = inner % 80 // 8 * 2 + inner // 80 - NW * ESTEP
    aim = jnp.where(inner < COLS, energy - column // 256 + shift, -100)
    for k in range(NM):
        reached = jnp.zeros(shape, jnp.int32)
        for place in range(NM):
            reached = jnp.where(q == place, table_ref[k, place], reached)
        same = inner % 8 == reached
        for x in range(NX):
            chosen = jnp.where(same & (aim == 2 * x), 1.0, 0.0)
            out_ref[k * 32 : (k + 1) * 32, x * 512 : (x + 1) * 512] = chosen.astype(jnp.bfloat16)


def column_choice(momentum_table):
    return pl.pallas_call(
        choice_kernel,
        out_shape=jax.ShapeDtypeStruct((NM * 32, NX * 512), jnp.bfloat16),
        in_specs=[pl.BlockSpec(memory_space=pltpu.SMEM)],
        out_specs=pl.BlockSpec(memory_space=pltpu.VMEM),
        cost_estimate=pl.CostEstimate(flops=1 << 24, bytes_accessed=1 << 20, transcendentals=0),
        compiler_params=pltpu.CompilerParams(vmem_limit_bytes=4 << 20),
    )(momentum_table)


def weights_kernel(data_ref, choice_ref, out_ref, factors_ref):
    lane = lax.broadcasted_iota(jnp.int32, (NM, 256), 1)
    mine = lane // 32 == lax.broadcasted_iota(jnp.int32, (NM, 256), 0)
    lane = lax.broadcasted_iota(jnp.int32, (NO, 256), 1)
    in_row = lane // NO == lax.broadcasted_iota(jnp.int32, (NO, 256), 0)
    entry = lax.broadcasted_iota(jnp.int32, (256, 512), 0) % NO
    lane = lax.broadcasted_iota(jnp.int32, (256, 512), 1)
    taken = jnp.where(lane < 256, lane // NO, lane % NO)
    pick = jnp.where(entry == taken, 1.0, 0.0).astype(jnp.bfloat16)

    def some_pairs(step, carry):
        at = pl.multiple_of(step * CHUNK, CHUNK)
        kept = data_ref[pl.ds(at, CHUNK), 256:512].astype(jnp.float32)
        rows = [jnp.where(mine, kept[i : i + 1, :], 0.0) for i in range(CHUNK)]
        spread = jnp.concatenate(rows, axis=0).astype(jnp.bfloat16)
        for x in range(NX):
            both = [
                jnp.dot(
                    spread,
                    choice_ref[:, (2 * x + b) * 256 : (2 * x + b + 1) * 256],
                    preferred_element_type=jnp.float32,
                ).reshape(CHUNK, NM, 256)
                for b in range(2)
            ]
            out_ref[pl.ds(at, CHUNK), x * 16 : (x + 1) * 16, :] = jnp.concatenate(
                both, axis=1
            ).astype(jnp.bfloat16)
        grads = data_ref[pl.ds(at, CHUNK), :256].astype(jnp.float32)
        rows = [jnp.where(in_row, grads[i : i + 1, :], 0.0) for i in range(CHUNK)]
        factors_ref[pl.ds(pl.multiple_of(at * NO, CHUNK * NO), CHUNK * NO), :] = jnp.dot(
            jnp.concatenate(rows, axis=0).astype(jnp.bfloat16),
            pick,
            preferred_element_type=jnp.float32,
        )
        return carry

    lax.fori_loop(0, BLOCK * NB // CHUNK, some_pairs, 0, unroll=4)


def weights_and_factors(data, choice):
    vmem = pl.BlockSpec(memory_space=pltpu.VMEM)
    return pl.pallas_call(
        weights_kernel,
        out_shape=[
            jax.ShapeDtypeStruct((BLOCK * NB, 64, 256), jnp.bfloat16),
            jax.ShapeDtypeStruct((BLOCK * NB * NO, 512), jnp.float32),
        ],
        in_specs=[vmem, vmem],
        out_specs=[vmem, vmem],
        cost_estimate=pl.CostEstimate(flops=1 << 30, bytes_accessed=6 << 20, transcendentals=0),
        compiler_params=pltpu.CompilerParams(vmem_limit_bytes=16 << 20),
    )(data, choice)


def atoms_kernel(begin, end, *refs):
    count = end - begin
    early = begin == 0
    if early:
        below_ref, own_ref, above_ref, weights_ref, factors_ref, out_ref, edge_ref = refs[:7]
        width, skip, known = EARLY, 0, 0
    else:
        below_ref, own_ref, above_ref, weights_ref, factors_ref, edge_ref, ready_ref, out_ref = refs[:8]
        width, skip, known = LATE, 2 * EARLY, 2 * REACH
    lanes, near, blend, sums = refs[-4:]
    stride, out_stride = 2 * width + 4, count + 2

    done = 0
    for part in (below_ref, own_ref, above_ref):
        at_row = skip if part is own_ref else 0

        def widen(i, carry, part=part, done=done, at_row=at_row):
            rows = part[i, at_row : at_row + 2 * width].astype(jnp.float32)
            at = pl.multiple_of((done + i) * stride, 4)
            for half in range(2):
                lanes[half, pl.ds(at, 2 * width), :] = rows[:, half * 128 : (half + 1) * 128]
            return carry

        lax.fori_loop(0, part.shape[0], widen, 0, unroll=4)
        done += part.shape[0]

    def regroup(place, carry):
        for b in range(2):
            for half in range(2):
                rows = lanes[half, pl.ds(place + b * width, 80, stride=stride), :]
                near[known + place, b * 80 : (b + 1) * 80, half * 128 : (half + 1) * 128] = (
                    rows.astype(jnp.bfloat16)
                )
        return carry

    lax.fori_loop(0, width, regroup, 0, unroll=4)
    if early:
        edge_ref[...] = near[count:]
    else:
        near[:known] = edge_ref[...]

    def blend_from(place, carry):
        bands = []
        for d, offset in enumerate(OFFSETS):
            atom = jnp.clip(begin + place - REACH - offset, 0, BLOCK - 1)
            bands.append(weights_ref[atom * NB + d][:, :COLS])
        mixed = jnp.dot(
            jnp.concatenate(bands, axis=0), near[place], preferred_element_type=jnp.float32
        ).astype(jnp.bfloat16)
        for d, offset in enumerate(OFFSETS):
            blend[(place - offset + REACH) * NB + d] = mixed[64 * d : 64 * (d + 1)]
        return carry

    lax.fori_loop(0, count + 2 * REACH, blend_from, 0, unroll=7 if early else 6)

    def one_atom(atom):
        total = jnp.zeros((64, 256), jnp.float32)
        for d in range(NB):
            row = pl.multiple_of(((begin + atom) * NB + d) * NO, NO)
            factors = factors_ref[pl.ds(row, NO), :]
            each, whole = factors[:, :256], factors[:, 256:]
            kron = jnp.concatenate(
                [(each[i : i + 1, :] * whole).astype(jnp.bfloat16) for i in range(NO)], axis=0
            )
            total = total + jnp.dot(
                blend[(atom + 2 * REACH) * NB + d], kron, preferred_element_type=jnp.float32
            )
        for x in range(NX):
            for b in range(2):
                row = x * 16 + b * 8
                at = (x * 16 + b) * out_stride + atom
                for half in range(2):
                    sums[half, pl.ds(at, NM, stride=2 * out_stride), :] = total[
                        row : row + NM, half * 128 : (half + 1) * 128
                    ]

    def some_atoms(step, carry):
        for i in range(UNROLL):
            one_atom(step * UNROLL + i)
        return carry

    lax.fori_loop(0, count // UNROLL, some_atoms, 0)

    def narrow(i, carry):
        for b in range(2):
            at = pl.multiple_of((2 * i + b) * out_stride, 2)
            rows = [sums[half, pl.ds(at, count), :] for half in range(2)]
            rows = jnp.concatenate(rows, axis=1)
            if not early:
                before = ready_ref[i, b * BLOCK : (b + 1) * BLOCK, :].astype(jnp.float32)
                rows = jnp.concatenate([before[:begin], rows], axis=0)
            out_ref[i, b * BLOCK : b * BLOCK + end, :] = rows.astype(jnp.bfloat16)
        return carry

    lax.fori_loop(0, NX * NM, narrow, 0, unroll=4)


def self_energy_of(begin, end, *operands):
    vmem = pl.BlockSpec(memory_space=pltpu.VMEM)
    count = end - begin
    width = EARLY if begin == 0 else LATE
    flops = 2 * count * NB * 64 * (COLS + 256) * 256
    out = jax.ShapeDtypeStruct((NX * NM, 2 * BLOCK, 256), jnp.bfloat16)
    edge = jax.ShapeDtypeStruct((2 * REACH, COLS, 256), jnp.bfloat16)
    return pl.pallas_call(
        functools.partial(atoms_kernel, begin, end),
        out_shape=[out, edge] if begin == 0 else out,
        in_specs=[vmem] * len(operands),
        out_specs=[vmem, vmem] if begin == 0 else vmem,
        scratch_shapes=[
            pltpu.VMEM((2, 80 * (2 * width + 4), 128), jnp.float32),
            pltpu.VMEM((count + 2 * REACH, COLS, 256), jnp.bfloat16),
            pltpu.VMEM(((count + 4 * REACH) * NB, 64, 256), jnp.bfloat16),
            pltpu.VMEM((2, 64 * (count + 2), 128), jnp.float32),
        ],
        cost_estimate=pl.CostEstimate(flops=flops, bytes_accessed=8 << 20, transcendentals=0),
        compiler_params=pltpu.CompilerParams(vmem_limit_bytes=20 << 20),
    )(*operands)


def body(green_blocks, neighbours, counts, couplings, grad_h, momentum_table):
    packed = packed_blocks(green_blocks.reshape(2, 1024, 256))
    packed, neighbours, counts, couplings, grad_h = lax.optimization_barrier(
        (packed, neighbours, counts, couplings, grad_h)
    )
    own = group_exchange(packed)
    up = [(i, i + 1) for i in range(NZ - 1)]
    down = [(b, a) for a, b in up]

    def exchanged(rows):
        below = lax.ppermute(own[NM:, rows], "z", up)
        above = lax.ppermute(own[:-NM, rows], "z", down)
        return below, above

    below, above = exchanged(slice(0, 2 * EARLY))
    held = atom_data(neighbours, counts, couplings, grad_h)
    choice = column_choice(momentum_table)
    held, own, choice = lax.optimization_barrier((held, own, choice))
    data = group_data(held)
    data, own = lax.optimization_barrier((data, own))
    late_below, late_above = exchanged(slice(2 * EARLY, 2 * WIDE_BLOCK))
    weights, factors = weights_and_factors(data, choice)
    result, edge = self_energy_of(
        0, FIRST, below, own, above, weights, factors
    )
    result = self_energy_of(
        FIRST, BLOCK, late_below, own, late_above, weights, factors, edge, result
    )
    back = group_exchange(result)
    back = back.reshape(NX, NM, 2, BLOCK, 256).transpose(2, 1, 0, 3, 4)
    return back.reshape(2, 1, 1024, 256)


def solution(mesh):
    cube = Mesh(mesh.devices.reshape(NZ, NX, NM), ("z", "x", "m"))
    flat = ("z", "x", "m")
    in_specs = (
        P(("z", "x"), "m", None, None),
        P(flat, None),
        P(flat),
        P(flat, None, None, None),
        P(flat, None, None, None),
        P(),
    )
    out_specs = P(("z", "x"), "m", None, None)
    return jax.shard_map(body, mesh=cube, in_specs=in_specs, out_specs=out_specs, check_vma=False)
```
